8 devices in a mesh: dp: 1 (over z), tp: 8 (over x, y, core).
Axes of the slice: x: 2, y: 2, z: 1, core: 2. Of those that a mesh axis runs over, the one named last changes fastest.
Arguments:
- x: bfloat16 [4096, 2048], P(('dp', 'tp'))
- dy: bfloat16 [4096, 2048], P(('dp', 'tp'))
- gain: bfloat16 [2048], replicated
- wq: bfloat16 [2048, 2048], P(None, 'tp')
- wk: bfloat16 [2048, 1024], P(None, 'tp')
- wv: bfloat16 [2048, 1024], P(None, 'tp')
- wo: bfloat16 [2048, 2048], P('tp')
Outputs:
- output 1: bfloat16 [4096, 2048], P(('dp', 'tp'))
- output 2: float32 [1, 2048], P('dp')
- output 3: bfloat16 [2048, 2048], P('dp', 'tp')
- output 4: bfloat16 [2048, 1024], P('dp', 'tp')
- output 5: bfloat16 [2048, 1024], P('dp', 'tp')
- output 6: bfloat16 [2048, 2048], P(('dp', 'tp'))
All inputs are finite; a program needn't handle non-finite values.
Results may differ from the reference program's by a relative error of at most 0.018.
Values are sent between devices in bfloat16 or wider.
A program may use at most 2 GiB of HBM per device.

```python
import jax
import jax.numpy as jnp
from jax import lax

ROWS = 4096
D = 2048
HEADS = 16
KV_HEADS = 8
HEAD = 128
THETA = 10000


def setup_inputs(seed: int = 0, part: int = 0) -> dict:
    kx, ky, kn, kq, kk, kv, ko = jax.random.split(jax.random.key(seed), 7)

    def weights(key, rows, columns):
        return jax.random.normal(key, (rows, columns), jnp.float32) * rows**-0.5

    drawn = {
        "x": jax.random.normal(jax.random.fold_in(kx, part), (ROWS, D), jnp.float32),
        "dy": jax.random.normal(jax.random.fold_in(ky, part), (ROWS, D), jnp.float32) * ROWS**-0.5,
        "gain": 1 + 0.1 * jax.random.normal(kn, (D,), jnp.float32),
        "wq": 2 * weights(kq, D, HEADS * HEAD),
        "wk": 2 * weights(kk, D, KV_HEADS * HEAD),
        "wv": 4 * weights(kv, D, KV_HEADS * HEAD),
        "wo": weights(ko, HEADS * HEAD, D),
    }
    return {k: v.astype(jnp.bfloat16) for k, v in drawn.items()}


def normed(x, gain):
    wide = x.astype(jnp.float32)
    scale = lax.rsqrt(jnp.mean(wide * wide, -1, keepdims=True) + 1e-6)
    return (wide * scale * gain.astype(jnp.float32)).astype(jnp.bfloat16)


def turned(t, place, theta):
    half = t.shape[-1] // 2
    angle = place.astype(jnp.float32)[:, None] * theta ** (-jnp.arange(half, dtype=jnp.float32) / half)
    cos, sin = jnp.cos(angle)[:, None], jnp.sin(angle)[:, None]
    a, b = t[..., :half].astype(jnp.float32), t[..., half:].astype(jnp.float32)
    return jnp.concatenate([a * cos - b * sin, b * cos + a * sin], -1).astype(jnp.bfloat16)


def matmul(a, w):
    return jnp.dot(a, w, preferred_element_type=jnp.float32).astype(jnp.bfloat16)


def einsum(form, a, b):
    return jnp.einsum(form, a.astype(jnp.float32), b.astype(jnp.float32))


def attention(q, k, v):
    scores = einsum("tgsd,ugd->gstu", q, k) * q.shape[-1] ** -0.5
    token = jnp.arange(q.shape[0])
    scores = jnp.where(token[:, None] >= token, scores, -jnp.inf)
    weights = jax.nn.softmax(scores, -1).astype(jnp.bfloat16)
    return einsum("gstu,ugd->tgsd", weights, v).astype(jnp.bfloat16)


def forward(x, gain, wq, wk, wv, wo):
    rows = x.shape[0]
    a, place = normed(x, gain), jnp.arange(rows)
    k = turned(matmul(a, wk).reshape(rows, -1, HEAD), place, THETA)
    q = turned(matmul(a, wq).reshape(rows, -1, HEAD), place, THETA).reshape(rows, k.shape[1], -1, HEAD)
    v = matmul(a, wv).reshape(rows, -1, HEAD)
    seen = attention(q, k, v).reshape(rows, -1)
    return (x.astype(jnp.float32) + jnp.dot(seen, wo, preferred_element_type=jnp.float32)).astype(jnp.bfloat16)


def reference(x, dy, gain, wq, wk, wv, wo):
    _, back = jax.vjp(forward, x, gain.astype(jnp.float32), wq, wk, wv, wo)
    by_x, by_gain, *by_weights = back(dy)
    return (by_x, by_gain[None], *by_weights)
```

```python
import jax
import jax.numpy as jnp
import numpy as np
from jax import lax
from jax.experimental import pallas as pl
from jax.experimental.pallas import tpu as pltpu
from jax.sharding import PartitionSpec as P

NEG = -1e30
HIDDEN = 2 * NEG
LOG2E = 1.4426950408889634
HEAD = 128
THETA = 10000
MESH = pl.DeviceIdType.MESH
BLK = 512
PIECES = 8
EPS = 1e-6
SCALE = HEAD**-0.5
E = SCALE * LOG2E


def _dot(a, b, ca, cb):
    return lax.dot_general(a, b, (((ca,), (cb,)), ((), ())), preferred_element_type=jnp.float32)


def flip(me, bit):
    return me + bit - 2 * bit * lax.rem(lax.div(me, bit), 2)


def rotary_tables(n):
    half = HEAD // 2
    rate = np.float64(np.float32(THETA) ** (-np.arange(half, dtype=np.float32) / np.float32(half)))
    rate = np.concatenate([rate, rate])[None]
    inner, outer = np.arange(BLK)[:, None] * rate, (BLK * np.arange(n))[:, None] * rate
    return [f(t).astype(np.float32) for t in (inner, outer) for f in (np.cos, np.sin)]


def gather_kernel(x_ref, dy_ref, gain_ref, wq_ref, wk_ref, wv_ref, wo_ref, ci_ref, si_ref, co_ref, so_ref,
                  a_ref, q_ref, k_ref, v_ref, do_ref, lse_ref, delta_ref, wt_ref, dwo_ref,
                  xs, dys, w_s, stage, o_s, dwo_s, top_s, mix_s, lsem, asem, ssem, rsem):
    me = lax.axis_index("tp")
    sib, yn, xn = flip(me, 1), flip(me, 2), flip(me, 4)
    dg = flip(yn, 4)
    rows = BLK // PIECES
    barrier = pltpu.get_barrier_semaphore()
    for t in (sib, xn, yn):
        pl.semaphore_signal(barrier, inc=1, device_id={"tp": t}, device_id_type=MESH)
    loads = [pltpu.make_async_copy(x_ref, xs.at[me], lsem.at[0]), pltpu.make_async_copy(dy_ref, dys.at[me], lsem.at[1]),
             pltpu.make_async_copy(wq_ref, w_s.at[:, pl.ds(0, 2 * HEAD)], lsem.at[2]),
             pltpu.make_async_copy(wk_ref, w_s.at[:, pl.ds(2 * HEAD, HEAD)], lsem.at[3]),
             pltpu.make_async_copy(wv_ref, w_s.at[:, pl.ds(3 * HEAD, HEAD)], lsem.at[4])]
    for c in loads:
        c.start()
    pl.semaphore_wait(barrier, 3)
    loads[0].wait()

    def copy(buf, n, kind, owner, p, to):
        part = buf.at[owner, pl.ds(p * rows, rows)]
        return pltpu.make_async_remote_copy(src_ref=part, dst_ref=part, send_sem=ssem.at[n, kind, p], recv_sem=rsem.at[n, kind, p],
                                            device_id={"tp": to}, device_id_type=MESH)

    def send_own(buf, n, p):
        copy(buf, n, 1, me, p, xn).start()
        copy(buf, n, 2, me, p, yn).start()

    def send_sib(buf, n):
        def go(p, _):
            copy(buf, n, 0, me, p, sib).start()
        lax.fori_loop(0, PIECES, go, None)

    def pass_on(buf, n, p):
        copy(buf, n, 1, xn, p, xn).wait_recv()
        copy(buf, n, 3, xn, p, sib).start()

        @pl.when(lax.rem(p, 2) == 0)
        def _():
            copy(buf, n, 5, xn, p, yn).start()

        copy(buf, n, 2, yn, p, yn).wait_recv()
        copy(buf, n, 4, yn, p, sib).start()

        @pl.when(lax.rem(p, 2) == 1)
        def _():
            copy(buf, n, 5, yn, p, xn).start()

    def pass_diagonal(buf, n, p):
        copy(buf, n, 5, dg, p, xn).wait_recv()
        copy(buf, n, 6, dg, p, sib).start()

    def arrived(buf, n, kind, owner):
        def go(p, _):
            copy(buf, n, kind, owner, p, sib).wait_recv()
        lax.fori_loop(0, PIECES, go, None)

    def owner_at(t):
        base = jnp.where(t < 2, me, jnp.where(t < 6, jnp.where(lax.rem(t, 2) == 0, xn, yn), dg))
        other = jnp.where(t < 2, t == 1, jnp.where(t < 6, t >= 4, t == 7))
        return jnp.where(other, flip(base, 1), base)

    def await_block(buf, n, t):
        @pl.when(t == 1)
        def _():
            arrived(buf, n, 0, sib)

        @pl.when((t >= 2) & (t < 6))
        def _():
            for u in range(2):
                pass_diagonal(buf, n, 2 * (t - 2) + u)

        @pl.when(t == 4)
        def _():
            arrived(buf, n, 3, flip(xn, 1))

        @pl.when(t == 5)
        def _():
            arrived(buf, n, 4, flip(yn, 1))

        @pl.when(t == 7)
        def _():
            arrived(buf, n, 6, flip(dg, 1))

    def first(p, _):
        send_own(xs, 0, p)
    lax.fori_loop(0, PIECES, first, None)
    send_sib(xs, 0)
    for c in loads[1:]:
        c.wait()

    def transpose(i, _):
        here = pl.ds(pl.multiple_of(i * 256, 256), 256)
        wt_ref[:, here] = w_s[here, :].T
    lax.fori_loop(0, w_s.shape[0] // 256, transpose, None)

    def put(t):
        slot = lax.rem(t, 2)
        return pltpu.make_async_copy(stage.at[slot], a_ref.at[owner_at(t)], asem.at[slot])

    def project(t, _):
        @pl.when(t == 2)
        def _():
            def go(p, _):
                pass_on(xs, 0, p)
            lax.fori_loop(0, PIECES, go, None)

        await_block(xs, 0, t)

        @pl.when((t >= 2) & (t < 6))
        def _():
            for u in range(2):
                send_own(dys, 1, 2 * (t - 2) + u)

        @pl.when(t >= 2)
        def _():
            put(t - 2).wait()

        owner, slot = owner_at(t), lax.rem(t, 2)
        gain = gain_ref[...].astype(jnp.float32)

        def norm(i, _):
            here = pl.ds(i * 64, 64)
            wide = xs[owner, here, :].astype(jnp.float32)
            s = lax.rsqrt(jnp.mean(wide * wide, -1, keepdims=True) + EPS)
            stage[slot, here, :] = (wide * s * gain).astype(jnp.bfloat16)
        lax.fori_loop(0, BLK // 64, norm, None)

        def multiply(i, _):
            here = pl.ds(pl.multiple_of(i * 256, 256), 256)
            there = pl.ds(pl.multiple_of(owner * BLK + i * 256, 256), 256)
            got = jnp.dot(stage[slot, here, :], w_s[...], preferred_element_type=jnp.float32)
            co, so = co_ref[pl.ds(owner, 1), :], so_ref[pl.ds(owner, 1), :]
            ci, si = ci_ref[here, :], si_ref[here, :]
            sign = jnp.where(lax.broadcasted_iota(jnp.int32, (1, HEAD), 1) < HEAD // 2, -1.0, 1.0)
            cos, sin = ci * co - si * so, (si * co + ci * so) * sign

            def turned(z):
                z = z.astype(jnp.bfloat16).astype(jnp.float32)
                return (z * cos + pltpu.roll(z, HEAD // 2, 1) * sin).astype(jnp.bfloat16)
            q_ref[0, there, :] = turned(got[:, :HEAD])
            q_ref[1, there, :] = turned(got[:, HEAD : 2 * HEAD])
            k_ref[there, :] = turned(got[:, 2 * HEAD : 3 * HEAD])
            v_ref[there, :] = got[:, 3 * HEAD :].astype(jnp.bfloat16)
        lax.fori_loop(0, BLK // 256, multiply, None)
        put(t).start()
    lax.fori_loop(0, 8, project, None)
    send_sib(dys, 1)

    ones = jnp.ones((8, BLK), jnp.bfloat16)

    def attend_rows(r, _):
        top_s[...] = jnp.full(top_s.shape, NEG, jnp.float32)
        mix_s[...] = jnp.zeros(mix_s.shape, jnp.float32)

        def block(j, strips, masked):
            here = pl.ds(pl.multiple_of(j * BLK, BLK), BLK)
            keys = k_ref[here, :]
            values = jnp.concatenate([v_ref[here, :].T, ones], axis=0)
            scores = [_dot(keys, q_ref[h, pl.ds(pl.multiple_of(r * 2 * BLK + half * BLK, BLK), BLK), :], 1, 1) for h, half in strips]
            weights, keeps = [], []
            for (h, half), s in zip(strips, scores):
                n = 2 * h + half
                if half in masked:
                    seen = lax.broadcasted_iota(jnp.int32, (BLK, BLK), 0) <= lax.broadcasted_iota(jnp.int32, (BLK, BLK), 1)
                    s = jnp.where(seen, s, HIDDEN)
                old = top_s[n : n + 1, :]
                top = jnp.maximum(old, s.max(axis=0, keepdims=True))
                top_s[n : n + 1, :] = top
                weights.append(jnp.exp2((s - top) * E).astype(jnp.bfloat16))
                keeps.append(jnp.exp2((old - top) * E))
            for (h, half), p, keep in zip(strips, weights, keeps):
                n = 2 * h + half
                mix_s[n] = mix_s[n] * keep + _dot(values, p, 1, 0)

        every = [(0, 0), (0, 1), (1, 0), (1, 1)]
        lax.fori_loop(0, 2 * r, lambda j, _: block(j, every, ()), None)
        block(2 * r, every, (0,))
        block(2 * r + 1, [(0, 1), (1, 1)], (1,))
        for h, half in every:
            n = 2 * h + half
            total = mix_s[n, HEAD : HEAD + 1, :]
            there = pl.ds(pl.multiple_of(r * 2 * BLK + half * BLK, BLK), BLK)
            o_s[there, h * HEAD : (h + 1) * HEAD] = (mix_s[n, :HEAD, :] * (1 / total)).T.astype(jnp.bfloat16)
            lse_ref[pl.ds(2 * r + half, 1), h * BLK : (h + 1) * BLK] = top_s[n : n + 1, :] * E + jnp.log2(total)
        for u in range(2):
            pass_on(dys, 1, 2 * r + u)
    lax.fori_loop(0, 4, attend_rows, None)

    dwo_s[...] = jnp.zeros(dwo_s.shape, jnp.float32)

    def back_out(t, _):
        await_block(dys, 1, t)
        owner = owner_at(t)
        there = pl.ds(pl.multiple_of(owner * BLK, BLK), BLK)
        got = _dot(dys[owner], wo_ref[...], 1, 1).astype(jnp.bfloat16)
        o = o_s[there, :]
        prod = got.astype(jnp.float32) * o.astype(jnp.float32)
        for h in range(2):
            do_ref[h, there, :] = got[:, h * HEAD : (h + 1) * HEAD]
            delta_ref[pl.ds(owner, 1), h * BLK : (h + 1) * BLK] = prod[:, h * HEAD : (h + 1) * HEAD].T.sum(axis=0, keepdims=True)
        dwo_s[...] += _dot(o, dys[owner], 0, 0)
    lax.fori_loop(0, 8, back_out, None)
    dwo_ref[...] = dwo_s[...].astype(jnp.bfloat16)

    for t in (6, 7):
        put(t).wait()

    def drain(p, _):
        for n, buf in ((0, xs), (1, dys)):
            for kind in range(7):
                copy(buf, n, kind, me, p, sib).wait_send()
    lax.fori_loop(0, PIECES, drain, None)


def gather_stage(x, dy, gain, wq, wk, wv, wo):
    n = 8
    tables = [jnp.asarray(t) for t in rotary_tables(n)]
    rows, d = n * BLK, x.shape[1]
    hbm, vmem = pl.BlockSpec(memory_space=pl.ANY), pl.BlockSpec(memory_space=pltpu.VMEM)
    low, f32 = jnp.bfloat16, jnp.float32
    sds = jax.ShapeDtypeStruct
    return pl.pallas_call(
        gather_kernel,
        out_shape=[sds((n, BLK, d), low), sds((2, rows, HEAD), low), sds((rows, HEAD), low), sds((rows, HEAD), low), sds((2, rows, HEAD), low),
                   sds((n, 2 * BLK), f32), sds((n, 2 * BLK), f32), sds((4 * HEAD, d), low), sds((2 * HEAD, d), low)],
        in_specs=[hbm, hbm, vmem, hbm, hbm, hbm, vmem, vmem, vmem, vmem, vmem],
        out_specs=[hbm] + [vmem] * 8,
        scratch_shapes=[pltpu.VMEM((n, BLK, d), low), pltpu.VMEM((n, BLK, d), low), pltpu.VMEM((d, 4 * HEAD), low), pltpu.VMEM((2, BLK, d), low),
                        pltpu.VMEM((rows, 2 * HEAD), low), pltpu.VMEM((2 * HEAD, d), f32), pltpu.VMEM((4, BLK), f32),
                        pltpu.VMEM((4, HEAD + 8, BLK), f32), pltpu.SemaphoreType.DMA((5,)), pltpu.SemaphoreType.DMA((2,)),
                        pltpu.SemaphoreType.DMA((2, 7, PIECES)), pltpu.SemaphoreType.DMA((2, 7, PIECES))],
        compiler_params=pltpu.CompilerParams(collective_id=0, has_side_effects=True, vmem_limit_bytes=67043328),
        name="gather_stage",
    )(x, dy, gain[None], wq, wk, wv, wo, *tables)


TURNS = (0, 7, 2, 5, 1, 6, 3, 4)
HALF = BLK // 2


def turn_at(n):
    got = jnp.int32(TURNS[0])
    for i in range(1, len(TURNS)):
        got = jnp.where(n == i, TURNS[i], got)
    return got


def scatter_kernel(x_ref, dy_ref, gain_ref, w_ref, q_ref, k_ref, v_ref, do_ref, lse_ref, delta_ref, a_ref, ci_ref, si_ref, co_ref, so_ref,
                   dx_ref, dgain_ref, dwq_ref, dwk_ref, dwv_ref,
                   dq_s, dk_s, dv_s, both_s, own_s, from_sib, relay, fin, terms, a_s, gains, lsem, asem, ssem, rsem, gsend, grecv):
    me = lax.axis_index("tp")
    sib, yn, xn = flip(me, 1), flip(me, 2), flip(me, 4)
    low, f32 = jnp.bfloat16, jnp.float32
    d = dx_ref.shape[1]
    barrier = pltpu.get_barrier_semaphore()
    for n in range(1, 8):
        pl.semaphore_signal(barrier, inc=1, device_id={"tp": lax.rem(me + n, 8)}, device_id_type=MESH)
    dq_s[...] = jnp.zeros(dq_s.shape, f32)
    dk_s[...] = jnp.zeros(dk_s.shape, f32)
    dv_s[...] = jnp.zeros(dv_s.shape, f32)
    pl.semaphore_wait(barrier, 7)

    def at(block):
        return pl.ds(pl.multiple_of(block * BLK, BLK), BLK)

    def blocks(pairs):
        work = [(h, n) for n in range(len(pairs)) for h in range(2)]
        keys = [k_ref[at(kb), :] for _, kb, _ in pairs]
        values = [v_ref[at(kb), :] for _, kb, _ in pairs]
        qs = [q_ref[h, at(pairs[n][0]), :] for h, n in work]
        dos = [do_ref[h, at(pairs[n][0]), :] for h, n in work]
        scores = [_dot(keys[n], z, 1, 1) for (h, n), z in zip(work, qs)]
        dps = [_dot(values[n], z, 1, 1) for (h, n), z in zip(work, dos)]
        ps, dss = [], []
        for (h, n), s, dp in zip(work, scores, dps):
            qb, kb, masked = pairs[n]
            p = jnp.exp2(s * E - lse_ref[pl.ds(qb, 1), h * BLK : (h + 1) * BLK])
            if masked:
                seen = lax.broadcasted_iota(jnp.int32, (BLK, BLK), 0) <= lax.broadcasted_iota(jnp.int32, (BLK, BLK), 1)
                p = jnp.where(seen, p, 0.0)
            ds = (p * (dp - delta_ref[pl.ds(qb, 1), h * BLK : (h + 1) * BLK])).astype(low)
            p = p.astype(low)
            dq_s[pl.ds(pl.multiple_of(qb * 2 * HEAD + h * HEAD, HEAD), HEAD), :] += _dot(keys[n].T, ds, 1, 0)
            ps.append(p)
            dss.append(ds)
            if h:
                dv_s[at(kb), :] += _dot(ps[-2], dos[len(ps) - 2], 1, 0) + _dot(p, dos[len(ps) - 1], 1, 0)
                dk_s[at(kb), :] += _dot(dss[-2], qs[len(ps) - 2], 1, 0) + _dot(ds, qs[len(ps) - 1], 1, 0)

    def finish(i):
        co, so = co_ref[pl.ds(i, 1), :], so_ref[pl.ds(i, 1), :]
        ci, si = ci_ref[...], si_ref[...]
        sign = jnp.where(lax.broadcasted_iota(jnp.int32, (1, HEAD), 1) < HEAD // 2, -1.0, 1.0)
        cos, sin = ci * co - si * so, (si * co + ci * so) * sign

        def turned_back(z):
            z = z * SCALE
            return (z * cos + pltpu.roll(z * sin, HEAD // 2, 1)).astype(low)
        for h in range(2):
            rows = pl.ds(pl.multiple_of(i * 2 * HEAD + h * HEAD, HEAD), HEAD)
            both_s[i, :, h * HEAD : (h + 1) * HEAD] = turned_back(dq_s[rows, :].T)
        both_s[i, :, 2 * HEAD : 3 * HEAD] = turned_back(dk_s[at(i), :])
        both_s[i, :, 3 * HEAD :] = dv_s[at(i), :].astype(low)

    def where(i):
        there, here = lax.div(i, 2), lax.div(me, 2)
        far_x = lax.rem(lax.div(there, 2) + lax.div(here, 2), 2)
        far_y = lax.rem(there + here, 2)
        return 2 * far_x + far_y, lax.rem(i + me, 2) == 0

    def half_rows(half):
        return pl.ds(pl.multiple_of(half * HALF, HALF), HALF)

    def term(i, half, put):
        def go(c, _):
            columns = pl.ds(pl.multiple_of(c * BLK, BLK), BLK)
            put(columns, jnp.dot(both_s[i, half_rows(half), :], w_ref[:, columns], preferred_element_type=f32))
        lax.fori_loop(0, d // BLK, go, None)

    def copy(kind, src, dst, n, to):
        return pltpu.make_async_remote_copy(src_ref=src, dst_ref=dst, send_sem=ssem.at[kind, n], recv_sem=rsem.at[kind, n],
                                            device_id={"tp": to}, device_id_type=MESH)

    def to_sib(slot, place, half):
        return copy(0, terms.at[slot, half_rows(half)], from_sib.at[place, half_rows(half)], 2 * place + half, sib)

    def to_x(half):
        return copy(1, from_sib.at[2, half_rows(half)], fin.at[0, half_rows(half)], half, xn)

    def to_y(half):
        return copy(2, from_sib.at[1, half_rows(half)], fin.at[1, half_rows(half)], half, yn)

    def round_x():
        return copy(3, from_sib.at[3, half_rows(0)], relay.at[0], 0, xn)

    def round_y():
        return copy(3, from_sib.at[3, half_rows(1)], relay.at[1], 1, yn)

    def offer(t):
        i = turn_at(t)
        place, mine = where(i)
        slot = lax.rem(lax.div(t, 2), 2)

        @pl.when(jnp.logical_not(mine))
        def _():
            for half in range(2):
                def put(columns, z, half=half):
                    terms[slot, half_rows(half), columns] = z.astype(low)
                term(i, half, put)
            for half in range(2):
                to_sib(slot, place, half).start()

    def left(t):
        place, mine = where(turn_at(t))

        @pl.when(jnp.logical_not(mine))
        def _():
            for half in range(2):
                to_sib(0, place, half).wait_send()

    def add(i, place, half, relayed):
        def put(columns, z):
            z = z + from_sib[place, half_rows(half), columns].astype(f32)
            if relayed:
                z = z + relay[half, :, columns].astype(f32)
            from_sib[place, half_rows(half), columns] = z.astype(low)
        term(i, half, put)

    def gather(t):
        i = turn_at(t)
        place, mine = where(i)

        @pl.when(mine)
        def _():
            for half in range(2):
                to_sib(0, place, half).wait_recv()

            @pl.when(place == 0)
            def _():
                for half in range(2):
                    def put(columns, z, half=half):
                        own_s[half_rows(half), columns] = z + from_sib[0, half_rows(half), columns].astype(f32)
                    term(i, half, put)

            @pl.when(place == 3)
            def _():
                for half in range(2):
                    add(i, 3, half, False)
                round_x().start()
                round_y().start()

            @pl.when(place == 1)
            def _():
                add(i, 1, 1, False)
                to_y(1).start()

            @pl.when(place == 2)
            def _():
                add(i, 2, 0, False)
                to_x(0).start()

    def pass_on(t):
        i = turn_at(t)
        place, mine = where(i)

        @pl.when(mine & (place == 1))
        def _():
            round_x().wait_recv()
            add(i, 1, 0, True)
            to_y(0).start()

        @pl.when(mine & (place == 2))
        def _():
            round_y().wait_recv()
            add(i, 2, 1, True)
            to_x(1).start()

    def turn(t, _):
        i = turn_at(t)

        def pair(c):
            return jnp.maximum(i, c), jnp.minimum(i, c), False

        @pl.when(lax.rem(t, 2) == 0)
        def _():
            @pl.when(t < 7)
            def _():
                blocks([(i, i, True), pair(turn_at(t + 1))])

        @pl.when(lax.rem(t, 2) == 1)
        def _():
            blocks([(i, i, True)])

        start = t + 2 - lax.rem(t, 2)

        def two(m, _):
            blocks([pair(turn_at(start + 2 * m)), pair(turn_at(start + 2 * m + 1))])
        lax.fori_loop(0, lax.div(7 - t, 2), two, None)
        finish(i)

        @pl.when(t >= 2)
        def _():
            left(t - 2)
        offer(t)

        @pl.when(t >= 1)
        def _():
            gather(t - 1)

        @pl.when((t >= 2) & (t < 6))
        def _():
            pass_on(t - 2)
    lax.fori_loop(0, 8, turn, None)

    def load(n):
        return pltpu.make_async_copy(a_ref.at[n], a_s.at[lax.rem(n, 2)], asem.at[lax.rem(n, 2)])

    load(0).start()
    gather(7)
    dq_s[...] = jnp.zeros(dq_s.shape, f32)

    def weights(n, _):
        @pl.when(n < 7)
        def _():
            load(n + 1).start()
        load(n).wait()

        def go(c, _):
            rows = pl.ds(pl.multiple_of(c * BLK, BLK), BLK)
            dq_s[rows, :] += _dot(a_s[lax.rem(n, 2), :, rows], both_s[n], 0, 0)
        lax.fori_loop(0, d // BLK, go, None)

        @pl.when(lax.rem(n, 2) == 1)
        def _():
            pass_on(4 + lax.div(n, 2))
    lax.fori_loop(0, 8, weights, None)
    dwq_ref[...] = dq_s[:, : 2 * HEAD].astype(low)
    dwk_ref[...] = dq_s[:, 2 * HEAD : 3 * HEAD].astype(low)
    dwv_ref[...] = dq_s[:, 3 * HEAD :].astype(low)

    left(6)
    left(7)
    mine = [pltpu.make_async_copy(x_ref, terms.at[0], lsem.at[0]), pltpu.make_async_copy(dy_ref, terms.at[1], lsem.at[1])]
    for c in mine:
        c.start()
    for c in mine:
        c.wait()
    gain = gain_ref[...].astype(f32)

    def last(half):
        to_x(half).wait_recv()
        to_y(half).wait_recv()

        def go(r, total):
            here = pl.ds(pl.multiple_of(half * HALF + r * 32, 32), 32)
            da = own_s[here, :] + fin[0, here, :].astype(f32) + fin[1, here, :].astype(f32)
            wide = terms[0, here, :].astype(f32)
            s = lax.rsqrt(jnp.mean(wide * wide, -1, keepdims=True) + EPS)
            hat = wide * s
            by_hat = da * hat
            z = da * gain
            dx = s * (z - hat * jnp.mean(z * hat, -1, keepdims=True))
            dx_ref[here, :] = (dx + terms[1, here, :].astype(f32)).astype(low)
            return total + by_hat.reshape(4, 8, d).sum(0)
        return lax.fori_loop(0, HALF // 32, go, jnp.zeros((8, d), f32))

    total = last(0) + last(1)
    gains[me] = total.sum(0, keepdims=True)

    def tell(n, slot):
        to = lax.rem(me + n, 8)
        return pltpu.make_async_remote_copy(src_ref=gains.at[slot], dst_ref=gains.at[slot], send_sem=gsend.at[n], recv_sem=grecv.at[n],
                                            device_id={"tp": to}, device_id_type=MESH)
    for n in range(1, 8):
        tell(n, me).start()
    for half in range(2):
        to_x(half).wait_send()
        to_y(half).wait_send()
    round_x().wait_send()
    round_y().wait_send()
    for n in range(1, 8):
        tell(n, lax.rem(me - n + 8, 8)).wait_recv()
    dgain_ref[...] = gains[...].sum(0)
    for n in range(1, 8):
        tell(n, me).wait_send()


def scatter_stage(x, dy, gain, w, q, k, v, do, lse, delta, a):
    n = 8
    tables = [jnp.asarray(t) for t in rotary_tables(n)]
    rows, d = n * BLK, x.shape[1]
    hbm, vmem = pl.BlockSpec(memory_space=pl.ANY), pl.BlockSpec(memory_space=pltpu.VMEM)
    low, f32 = jnp.bfloat16, jnp.float32
    sds = jax.ShapeDtypeStruct
    sem = pltpu.SemaphoreType.DMA
    return pl.pallas_call(
        scatter_kernel,
        out_shape=[sds((BLK, d), low), sds((1, d), f32), sds((d, 2 * HEAD), low), sds((d, HEAD), low), sds((d, HEAD), low)],
        in_specs=[hbm, hbm] + [vmem] * 8 + [hbm] + [vmem] * 4,
        out_specs=[vmem] * 5,
        scratch_shapes=[pltpu.VMEM((d, 4 * HEAD), f32), pltpu.VMEM((rows, HEAD), f32), pltpu.VMEM((rows, HEAD), f32),
                        pltpu.VMEM((n, BLK, 4 * HEAD), low), pltpu.VMEM((BLK, d), f32), pltpu.VMEM((4, BLK, d), low),
                        pltpu.VMEM((2, HALF, d), low), pltpu.VMEM((2, BLK, d), low), pltpu.VMEM((2, BLK, d), low),
                        pltpu.VMEM((2, BLK, d), low), pltpu.VMEM((n, 1, d), f32), sem((2,)), sem((2,)), sem((4, 8)), sem((4, 8)),
                        sem((n,)), sem((n,))],
        compiler_params=pltpu.CompilerParams(collective_id=1, has_side_effects=True, vmem_limit_bytes=67043328),
        name="scatter_stage",
    )(x, dy, gain[None], w, q, k, v, do, lse, delta, a, *tables)


def solution(mesh):
    def step(x, dy, gain, wq, wk, wv, wo):
        a, q, k, v, do, lse, delta, w, dwo = gather_stage(x, dy, gain, wq, wk, wv, wo)
        dx, dgain, dwq, dwk, dwv = scatter_stage(x, dy, gain, w, q, k, v, do, lse, delta, a)
        return dx, dgain, dwq, dwk, dwv, dwo

    tokens, columns = P(("dp", "tp"), None), P(None, "tp")
    return jax.shard_map(
        step,
        mesh=mesh,
        in_specs=(tokens, tokens, P(None), columns, columns, columns, P("tp", None)),
        out_specs=(tokens, P("dp", None), P("dp", "tp"), P("dp", "tp"), P("dp", "tp"), P(("dp", "tp"), None)),
        check_vma=False,
    )
```

```python
import jax
import jax.numpy as jnp
import numpy as np
from jax import lax
from jax.experimental import pallas as pl
from jax.experimental.pallas import tpu as pltpu
from jax.sharding import PartitionSpec as P

NEG = -1e30
HIDDEN = 2 * NEG
LOG2E = 1.4426950408889634
HEAD = 128
THETA = 10000
MESH = pl.DeviceIdType.MESH
UNROLL = 2
DEVICES = 8
WIDE = 2 * HEAD
BLK = 512
MIX = HEAD + 8
PIECES = 8
EPS = 1e-6
SCALE = HEAD**-0.5
E = SCALE * LOG2E


def _dot(a, b, ca, cb):
    return lax.dot_general(a, b, (((ca,), (cb,)), ((), ())), preferred_element_type=jnp.float32)


def dot(a, b):
    return _dot(a, b, 1, 0)


def dot_rows(a, b):
    return _dot(a, b, 1, 1)


def dot_columns(a, b):
    return _dot(a, b, 0, 0)


def pair_of(n):
    return lax.div(n, 2)


def parity(n):
    return lax.rem(n, 2)


def repeat(times, body, unroll=1):
    lax.fori_loop(0, times, body, None, unroll=unroll)


def flip(me, bit):
    return me + bit - 2 * bit * parity(lax.div(me, bit))


def rotary_tables(n):
    half = HEAD // 2
    rate = np.float64(np.float32(THETA) ** (-np.arange(half, dtype=np.float32) / np.float32(half)))
    rate = np.concatenate([rate, rate])[None]
    inner, outer = np.arange(BLK)[:, None] * rate, (BLK * np.arange(n))[:, None] * rate
    return [f(t).astype(np.float32) for t in (inner, outer) for f in (np.cos, np.sin)]


TURNS = (0, 7, 2, 5, 1, 6, 3, 4)
HALF = BLK // 2
QUARTER = BLK // 4
AHEAD = 1


def turn_at(n):
    got = jnp.int32(TURNS[0])
    for i in range(1, len(TURNS)):
        got = jnp.where(n == i, TURNS[i], got)
    return got


def layer_kernel(x_ref, dy_ref, gain_ref, wq_ref, wk_ref, wv_ref, wo_ref, ci_ref, si_ref, co_ref, so_ref,
                 a_ref, dx_ref, dgain_ref, dwq_ref, dwk_ref, dwv_ref, dwo_ref,
                 xs, dys, stage, q_s, k_s, v_s, do_s, lse_s, delta_s, wide_s, top_s, dq_s, dk_s, dv_s, gains,
                 lsem, asem, ssem, rsem, ssem2, rsem2, gsend, grecv, ready):
    low, f32 = jnp.bfloat16, jnp.float32
    d = x_ref.shape[1]
    me = lax.axis_index("tp")
    sib, yn, xn = flip(me, 1), flip(me, 2), flip(me, 4)
    dg = flip(yn, 4)
    rows = BLK // PIECES
    barrier = pltpu.get_barrier_semaphore()
    for n in range(1, DEVICES):
        pl.semaphore_signal(barrier, inc=1, device_id={"tp": lax.rem(me + n, DEVICES)}, device_id_type=MESH)
    loads = [pltpu.make_async_copy(x_ref, xs.at[me], lsem.at[0]), pltpu.make_async_copy(dy_ref, dys.at[me], lsem.at[1]),
             pltpu.make_async_copy(wq_ref.at[:, pl.ds(0, HEAD)], do_s.at[0, pl.ds(0, d)], lsem.at[2]),
             pltpu.make_async_copy(wq_ref.at[:, pl.ds(HEAD, HEAD)], do_s.at[0, pl.ds(d, d)], lsem.at[3]),
             pltpu.make_async_copy(wk_ref, do_s.at[1, pl.ds(0, d)], lsem.at[4]),
             pltpu.make_async_copy(wv_ref, do_s.at[1, pl.ds(d, d)], lsem.at[5])]
    for c in loads:
        c.start()
    pl.semaphore_wait(barrier, 7)
    loads[0].wait()

    def copy(buf, n, kind, owner, p, to):
        part = buf.at[owner, pl.ds(p * rows, rows)]
        return pltpu.make_async_remote_copy(src_ref=part, dst_ref=part, send_sem=ssem.at[n, kind, p], recv_sem=rsem.at[n, kind, p],
                                            device_id={"tp": to}, device_id_type=MESH)

    def send_own(buf, n, p):
        copy(buf, n, 1, me, p, xn).start()
        copy(buf, n, 2, me, p, yn).start()

    def send_sib(buf, n):
        def go(p, _):
            copy(buf, n, 0, me, p, sib).start()
        repeat(PIECES, go)

    def pass_on(buf, n, p):
        copy(buf, n, 1, xn, p, xn).wait_recv()
        copy(buf, n, 3, xn, p, sib).start()

        @pl.when(parity(p) == 0)
        def _():
            copy(buf, n, 5, xn, p, yn).start()

        copy(buf, n, 2, yn, p, yn).wait_recv()
        copy(buf, n, 4, yn, p, sib).start()

        @pl.when(parity(p) == 1)
        def _():
            copy(buf, n, 5, yn, p, xn).start()

    def pass_diagonal(buf, n, p):
        copy(buf, n, 5, dg, p, xn).wait_recv()
        copy(buf, n, 6, dg, p, sib).start()

    def arrived(buf, n, kind, owner):
        def go(p, _):
            copy(buf, n, kind, owner, p, sib).wait_recv()
        repeat(PIECES, go)

    def owner_at(t):
        base = jnp.where(t < 2, me, jnp.where(t < 6, jnp.where(parity(t) == 0, xn, yn), dg))
        other = jnp.where(t < 2, t == 1, jnp.where(t < 6, t >= 4, t == 7))
        return jnp.where(other, flip(base, 1), base)

    def await_block(buf, n, t):
        @pl.when(t == 1)
        def _():
            arrived(buf, n, 0, sib)

        @pl.when((t >= 3 - n) & (t < 7 - n))
        def _():
            for u in range(2):
                pass_diagonal(buf, n, 2 * (t - 3 + n) + u)

        @pl.when(t == 4)
        def _():
            arrived(buf, n, 3, flip(xn, 1))

        @pl.when(t == 5)
        def _():
            arrived(buf, n, 4, flip(yn, 1))

        @pl.when(t == 7)
        def _():
            arrived(buf, n, 6, flip(dg, 1))

    def first(p, _):
        send_own(xs, 0, p)
    repeat(PIECES, first)
    send_sib(xs, 0)
    for c in loads[1:]:
        c.wait()

    def put(t):
        slot = parity(t)
        return pltpu.make_async_copy(stage.at[slot], a_ref.at[owner_at(t)], asem.at[slot])

    def project(t, _):
        @pl.when(t == 2)
        def _():
            def go(p, _):
                pass_on(xs, 0, p)
            repeat(PIECES, go)

        await_block(xs, 0, t)

        @pl.when((t >= 2) & (t < 6))
        def _():
            for u in range(2):
                send_own(dys, 1, 2 * (t - 2) + u)

        @pl.when(t >= 2)
        def _():
            put(t - 2).wait()

        owner, slot = owner_at(t), parity(t)
        gain = gain_ref[...].astype(f32)

        def norm(i, _):
            here = pl.ds(i * 64, 64)
            wide = xs[owner, here, :].astype(jnp.float32)
            s = lax.rsqrt(jnp.mean(wide * wide, -1, keepdims=True) + EPS)
            stage[slot, here, :] = (wide * s * gain).astype(jnp.bfloat16)
        repeat(BLK // 64, norm)

        def multiply(i, _):
            here = pl.ds(pl.multiple_of(i * HALF, HALF), HALF)
            there = pl.ds(pl.multiple_of(owner * BLK + i * HALF, HALF), HALF)
            w = jnp.concatenate([do_s[h, n * d : (n + 1) * d, :] for h in range(2) for n in range(2)], axis=1)
            got = dot(stage[slot, here, :], w)
            co, so = co_ref[pl.ds(owner, 1), :], so_ref[pl.ds(owner, 1), :]
            ci, si = ci_ref[here, :], si_ref[here, :]
            sign = jnp.where(lax.broadcasted_iota(jnp.int32, (1, HEAD), 1) < HEAD // 2, -1.0, 1.0)
            cos, sin = ci * co - si * so, (si * co + ci * so) * sign

            def turned(z):
                z = z.astype(jnp.bfloat16).astype(jnp.float32)
                return (z * cos + pltpu.roll(z, HEAD // 2, 1) * sin).astype(jnp.bfloat16)
            q_s[0, there, :] = turned(got[:, :HEAD])
            q_s[1, there, :] = turned(got[:, HEAD : WIDE])
            k_s[there, :] = turned(got[:, WIDE : 3 * HEAD])
            v_s[there, :] = got[:, 3 * HEAD :].astype(jnp.bfloat16)
        repeat(BLK // HALF, multiply)
        put(t).start()
    repeat(DEVICES, project)
    send_sib(dys, 1)

    def drain(n, buf):
        def go(p, _):
            for kind in range(7):
                copy(buf, n, kind, me, p, sib).wait_send()
        repeat(PIECES, go)
    drain(0, xs)
    for t in (sib, xn, yn, flip(xn, 1), flip(yn, 1)):
        pl.semaphore_signal(ready, inc=1, device_id={"tp": t}, device_id_type=MESH)
    for t in (6, 7):
        put(t).wait()
    get_wo = pltpu.make_async_copy(wo_ref, stage.at[0, pl.ds(0, WIDE)], lsem.at[0])
    get_wo.start()

    ones = jnp.ones((8, BLK), jnp.bfloat16)

    def attend_rows(r, _):
        top_s[...] = jnp.full(top_s.shape, NEG, jnp.float32)
        dq_s[: 4 * MIX, :] = jnp.zeros((4 * MIX, BLK), f32)

        def block(j, strips, masked):
            here = pl.ds(pl.multiple_of(j * BLK, BLK), BLK)
            keys = k_s[here, :]
            values = jnp.concatenate([v_s[here, :].T, ones], axis=0)
            scores = [dot_rows(keys, q_s[h, pl.ds(pl.multiple_of(r * 2 * BLK + half * BLK, BLK), BLK), :]) for h, half in strips]
            weights, keeps = [], []
            for (h, half), s in zip(strips, scores):
                n = 2 * h + half
                if half in masked:
                    seen = lax.broadcasted_iota(jnp.int32, (BLK, BLK), 0) <= lax.broadcasted_iota(jnp.int32, (BLK, BLK), 1)
                    s = jnp.where(seen, s, HIDDEN)
                old = top_s[n : n + 1, :]
                top = jnp.maximum(old, s.max(axis=0, keepdims=True))
                top_s[n : n + 1, :] = top
                weights.append(jnp.exp2((s - top) * E).astype(jnp.bfloat16))
                keeps.append(jnp.exp2((old - top) * E))
            for (h, half), p, keep in zip(strips, weights, keeps):
                n = 2 * h + half
                here = pl.ds(n * MIX, MIX)
                dq_s[here, :] = dq_s[here, :] * keep + dot(values, p)

        every = [(0, 0), (0, 1), (1, 0), (1, 1)]
        lax.fori_loop(0, 2 * r, lambda j, _: block(j, every, ()), None)
        block(2 * r, every, (0,))
        block(2 * r + 1, [(0, 1), (1, 1)], (1,))
        for h, half in every:
            n = 2 * h + half
            total = dq_s[n * MIX + HEAD : n * MIX + HEAD + 1, :]
            xs[7, :, pl.ds(pl.multiple_of((2 * r + half) * WIDE + h * HEAD, HEAD), HEAD)] = (dq_s[n * MIX : n * MIX + HEAD, :] * (1 / total)).T.astype(jnp.bfloat16)
            lse_s[pl.ds(2 * r + half, 1), h * BLK : (h + 1) * BLK] = top_s[n : n + 1, :] * E + jnp.log2(total)
        pass_on(dys, 1, r)
    repeat(4, attend_rows)

    get_wo.wait()
    def transpose(i, _):
        here = pl.ds(pl.multiple_of(i * HALF, HALF), HALF)
        for n in range(4):
            stage[1, n * HEAD : (n + 1) * HEAD, here] = do_s[n // 2, pl.ds(pl.multiple_of(n % 2 * d + i * HALF, HALF), HALF), :].T
    repeat(d // HALF, transpose)

    dq_s[...] = jnp.zeros(dq_s.shape, f32)
    dk_s[...] = jnp.zeros(dk_s.shape, f32)
    dv_s[...] = jnp.zeros(dv_s.shape, f32)
    wide_s[...] = jnp.zeros(wide_s.shape, f32)

    def at(block):
        return pl.ds(pl.multiple_of(block * BLK, BLK), BLK)

    def rows_of(block, part):
        return pl.ds(pl.multiple_of(block * BLK + part[0], HALF), part[1])

    def pieces(*todo):
        work = [(h, n) for n in range(len(todo)) for h in range(2)]
        keys = [k_s[rows_of(kb, kp), :] for _, kb, _, kp, _ in todo]
        values = [v_s[rows_of(kb, kp), :] for _, kb, _, kp, _ in todo]
        qs = [q_s[h, rows_of(todo[n][0], todo[n][2]), :] for h, n in work]
        dos = [do_s[h, rows_of(todo[n][0], todo[n][2]), :] for h, n in work]
        def products(i):
            h, n = work[i]
            return dot_rows(keys[n], qs[i]), dot_rows(values[n], dos[i])

        ready_at = [products(i) for i in range(min(AHEAD, len(work)))]
        for i, (h, n) in enumerate(work):
            if i + AHEAD < len(work):
                ready_at.append(products(i + AHEAD))
            s, dp = ready_at[i]
            ready_at[i] = None
            qb, kb, qp, kp, masked = todo[n]
            columns = pl.ds(h * BLK + qp[0], qp[1])
            p = jnp.exp2(s * E - lse_s[pl.ds(qb, 1), columns])
            if masked:
                seen = lax.broadcasted_iota(jnp.int32, s.shape, 0) + kp[0] <= lax.broadcasted_iota(jnp.int32, s.shape, 1) + qp[0]
                p = jnp.where(seen, p, 0.0)
            ds = (p * (dp - delta_s[pl.ds(qb, 1), columns])).astype(low)
            p = p.astype(low)
            dq_s[pl.ds(pl.multiple_of(qb * WIDE + h * HEAD, HEAD), HEAD), qp[0] : qp[0] + qp[1]] += dot(keys[n].T, ds)
            here = rows_of(kb, kp)
            dv_s[here, :] += dot(p, dos[i])
            dk_s[here, :] += dot(ds, qs[i])

    whole, upper, lower = (0, BLK), (0, HALF), (HALF, HALF)

    def two_blocks(a, b):
        pieces((*a, whole, whole, False), (*b, whole, whole, False))

    def one_block(q, k):
        pieces((q, k, whole, upper, False), (q, k, whole, lower, False))

    def diagonal_block(i):
        pieces((i, i, whole, upper, True), (i, i, lower, lower, True))

    def early(block):
        return (pair_of(block) == pair_of(me)) | (me < 4) & (block < 4) | (me < 2) & (block == 4) | (pair_of(me) == 2) & (block < 2)

    def back_out(t, _):
        @pl.when(t == 0)
        def _():
            pass_on(dys, 1, 4)

        @pl.when(t == 1)
        def _():
            pass_on(dys, 1, 5)

        @pl.when(t == 2)
        def _():
            pass_on(dys, 1, 6)
            pass_on(dys, 1, 7)
        await_block(dys, 1, t)
        owner = owner_at(t)
        there = at(owner)
        got = dot_rows(dys[owner], stage[0, : WIDE, :]).astype(low)
        o = xs[7, :, pl.ds(pl.multiple_of(owner * WIDE, WIDE), WIDE)]
        prod = got.astype(f32) * o.astype(f32)
        for h in range(2):
            do_s[h, there, :] = got[:, h * HEAD : (h + 1) * HEAD]
            delta_s[pl.ds(owner, 1), h * BLK : (h + 1) * BLK] = prod[:, h * HEAD : (h + 1) * HEAD].T.sum(axis=0, keepdims=True)
        wide_s[...] += dot_columns(o, dys[owner])

        @pl.when(early(owner))
        def _():
            def two(m, _):
                two_blocks((owner, 2 * m), (owner, 2 * m + 1))
            repeat(pair_of(owner), two)

            @pl.when(parity(owner) == 1)
            def _():
                one_block(owner, owner - 1)
            diagonal_block(owner)
    repeat(DEVICES, back_out)
    drain(1, dys)
    stage[0, : WIDE, :] = wide_s[...].astype(low)
    pl.semaphore_wait(ready, 5)
    by_wo = pltpu.make_async_copy(stage.at[0, pl.ds(0, WIDE)], dwo_ref, lsem.at[4])
    mine = [pltpu.make_async_copy(x_ref, dys.at[4], lsem.at[5]), pltpu.make_async_copy(dy_ref, dys.at[5], lsem.at[6])]
    for c in (by_wo, *mine):
        c.start()

    def part(i, n):
        return pl.ds(pl.multiple_of(lax.rem(i, 4) * BLK + n * HEAD, HEAD), HEAD)

    def all_of(i):
        return pl.ds(pl.multiple_of(lax.rem(i, 4) * BLK, BLK), BLK)

    def finish(i):
        co, so = co_ref[pl.ds(i, 1), :], so_ref[pl.ds(i, 1), :]
        ci, si = ci_ref[...], si_ref[...]
        sign = jnp.where(lax.broadcasted_iota(jnp.int32, (1, HEAD), 1) < HEAD // 2, -1.0, 1.0)
        cos, sin = ci * co - si * so, (si * co + ci * so) * sign

        def turned_back(z):
            z = z * SCALE
            return (z * cos + pltpu.roll(z * sin, HEAD // 2, 1)).astype(low)
        for h in range(2):
            rows = pl.ds(pl.multiple_of(i * WIDE + h * HEAD, HEAD), HEAD)
            dys[lax.div(i, 4), :, part(i, h)] = turned_back(dq_s[rows, :].T)
        dys[lax.div(i, 4), :, part(i, 2)] = turned_back(dk_s[at(i), :])
        dys[lax.div(i, 4), :, part(i, 3)] = dv_s[at(i), :].astype(low)

    core = parity(me)

    def where(i):
        there, here = pair_of(i), pair_of(me)
        far_x = parity(pair_of(there) + pair_of(here))
        far_y = parity(there + here)
        return 2 * far_x + far_y, parity(i)

    def half_rows(half):
        return pl.ds(pl.multiple_of(half * HALF, HALF), HALF)

    def quarter_rows(half, quarter):
        return pl.ds(pl.multiple_of(half * HALF + quarter * QUARTER, QUARTER), QUARTER)

    def term(i, rows, put):
        def go(c, _):
            columns = pl.ds(pl.multiple_of(c * BLK, BLK), BLK)
            put(columns, dot(dys[lax.div(i, 4), rows, all_of(i)], stage[1, :, columns]))
        repeat(d // BLK, go, UNROLL)

    def sum_copy(kind, src, dst, left_n, n, to):
        return pltpu.make_async_remote_copy(src_ref=src, dst_ref=dst, send_sem=ssem2.at[kind, left_n], recv_sem=rsem2.at[kind, n],
                                            device_id={"tp": to}, device_id_type=MESH)

    def to_sib(slot, half, place, landing):
        return sum_copy(0, dys.at[6 + slot, half_rows(half)], xs.at[place, half_rows(landing)], 2 * place + landing, 2 * place + landing, sib)

    def kept_by(neighbour, to):
        return pair_of(neighbour) * 2 + to

    def to_x(to, quarter):
        return sum_copy(1, xs.at[2, quarter_rows(to, quarter)], xs.at[4, quarter_rows(core, quarter)], 2 * to + quarter, 2 * core + quarter, kept_by(xn, to))

    def to_y(to, quarter):
        return sum_copy(2, xs.at[1, quarter_rows(to, quarter)], xs.at[5, quarter_rows(core, quarter)], 2 * to + quarter, 2 * core + quarter, kept_by(yn, to))

    def from_x(half, quarter):
        return sum_copy(1, xs.at[2, quarter_rows(half, quarter)], xs.at[4, quarter_rows(half, quarter)], 0, 2 * half + quarter, xn)

    def from_y(half, quarter):
        return sum_copy(2, xs.at[1, quarter_rows(half, quarter)], xs.at[5, quarter_rows(half, quarter)], 0, 2 * half + quarter, yn)

    def round_x(to):
        return sum_copy(3, xs.at[3, quarter_rows(to, 0)], xs.at[6, quarter_rows(to, 0)], 2 * to, 2 * to, xn)

    def round_y(to):
        return sum_copy(3, xs.at[3, quarter_rows(to, 1)], xs.at[6, quarter_rows(to, 1)], 2 * to + 1, 2 * to + 1, yn)

    def offer(t):
        i = turn_at(t)
        place, to = where(i)
        slot = parity(t)

        def give(half, landing):
            def put(columns, z):
                dys[6 + slot, half_rows(half), columns] = z.astype(low)
            term(i, half_rows(half), put)
            to_sib(slot, half, place, landing).start()

        @pl.when(place > 0)
        def _():
            give(1 - core, to)

        @pl.when((place == 0) & (to != core))
        def _():
            def both(half, _):
                give(half, half)
            repeat(2, both)

    def left(t):
        place, to = where(turn_at(t))

        @pl.when(place > 0)
        def _():
            to_sib(0, 0, place, to).wait_send()

        @pl.when((place == 0) & (to != core))
        def _():
            for half in range(2):
                to_sib(0, 0, 0, half).wait_send()

    def add(i, place, to, quarter, relayed):
        def put(columns, z):
            here = quarter_rows(to, quarter)
            z = z + xs[place, here, columns].astype(f32)
            if relayed:
                z = z + xs[6, here, columns].astype(f32)
            xs[place, here, columns] = z.astype(low)
        term(i, quarter_rows(core, quarter), put)

    def gather_sum(t):
        i = turn_at(t)
        place, to = where(i)

        @pl.when(place > 0)
        def _():
            to_sib(0, 0, place, to).wait_recv()

        @pl.when(place == 3)
        def _():
            def put(columns, z):
                xs[3, half_rows(to), columns] = (z + xs[3, half_rows(to), columns].astype(f32)).astype(low)
            term(i, half_rows(core), put)
            round_x(to).start()
            round_y(to).start()

        @pl.when(place == 1)
        def _():
            add(i, 1, to, 1, False)
            to_y(to, 1).start()

        @pl.when(place == 2)
        def _():
            add(i, 2, to, 0, False)
            to_x(to, 0).start()

    def pass_sum(t):
        i = turn_at(t)
        place, to = where(i)

        @pl.when(place == 1)
        def _():
            round_x(to).wait_recv()
            add(i, 1, to, 0, True)
            to_y(to, 0).start()

        @pl.when(place == 2)
        def _():
            round_y(to).wait_recv()
            add(i, 2, to, 1, True)
            to_x(to, 1).start()

    def turn(t, _):
        i = turn_at(t)

        @pl.when(jnp.logical_not(early(i)))
        def _():
            diagonal_block(i)

        def pair_with(c):
            return jnp.maximum(i, c), jnp.minimum(i, c)

        def others(m, held):
            c = turn_at(m)
            wanted = jnp.logical_not(early(jnp.maximum(i, c)))

            @pl.when(wanted & (held >= 0))
            def _():
                two_blocks(pair_with(held), pair_with(c))

            @pl.when((t >= 1) & (m == t + 3))
            def _():
                gather_sum(t - 1)
            return jnp.where(wanted, jnp.where(held >= 0, -1, c), held)
        held = lax.fori_loop(t + 1, DEVICES, others, jnp.int32(-1))

        @pl.when(held >= 0)
        def _():
            one_block(*pair_with(held))

        @pl.when(t >= 5)
        def _():
            gather_sum(t - 1)
        finish(i)

        @pl.when(t >= 2)
        def _():
            left(t - 2)
        offer(t)

        @pl.when((t >= 2) & (t < 7) & (parity(t) == 0))
        def _():
            pass_sum(pair_of(t) - 1)
    repeat(DEVICES, turn)

    def load(n):
        return pltpu.make_async_copy(a_ref.at[n], dys.at[2 + parity(n)], asem.at[parity(n)])

    load(0).start()
    gather_sum(7)
    pass_sum(3)
    dq_s[...] = jnp.zeros(dq_s.shape, f32)

    def weights(n, _):
        @pl.when(n < 7)
        def _():
            load(n + 1).start()

        @pl.when((n >= 1) & (n < 5))
        def _():
            pass_sum(n + 3)
        load(n).wait()

        def go(c, _):
            rows = pl.ds(pl.multiple_of(c * BLK, BLK), BLK)
            dq_s[rows, :] += dot_columns(dys[2 + parity(n), :, rows], dys[lax.div(n, 4), :, all_of(n)])
        repeat(d // BLK, go)
    repeat(DEVICES, weights)
    for n, half in enumerate((q_s.at[0], q_s.at[1], k_s, v_s)):
        half[:d, :] = dq_s[:, n * HEAD : (n + 1) * HEAD].astype(low)
    results = [pltpu.make_async_copy(q_s.at[0, pl.ds(0, d)], dwq_ref.at[:, pl.ds(0, HEAD)], lsem.at[0]),
               pltpu.make_async_copy(q_s.at[1, pl.ds(0, d)], dwq_ref.at[:, pl.ds(HEAD, HEAD)], lsem.at[1]),
               pltpu.make_async_copy(k_s.at[pl.ds(0, d)], dwk_ref, lsem.at[2]), pltpu.make_async_copy(v_s.at[pl.ds(0, d)], dwv_ref, lsem.at[3])]
    left(6)
    left(7)
    for c in results:
        c.start()
    for c in mine:
        c.wait()
    gain = gain_ref[...].astype(f32)

    def last(half):
        to_sib(0, 0, 0, half).wait_recv()
        for quarter in range(2):
            from_x(half, quarter).wait_recv()
            from_y(half, quarter).wait_recv()

        def add_up(columns, z):
            wide_s[:, columns] = z + sum(xs[n, half_rows(half), columns].astype(f32) for n in (0, 4, 5))
        term(me, half_rows(half), add_up)

        def go(r, total):
            here, there = pl.ds(pl.multiple_of(r * 32, 32), 32), pl.ds(pl.multiple_of(half * HALF + r * 32, 32), 32)
            da = wide_s[here, :]
            wide = dys[4, there, :].astype(f32)
            s = lax.rsqrt(jnp.mean(wide * wide, -1, keepdims=True) + EPS)
            hat = wide * s
            by_hat = da * hat
            z = da * gain
            dx = s * (z - hat * jnp.mean(z * hat, -1, keepdims=True))
            dys[5, there, :] = (dx + dys[5, there, :].astype(f32)).astype(low)
            return total + by_hat.reshape(4, 8, d).sum(0)
        return lax.fori_loop(0, HALF // 32, go, jnp.zeros((8, d), f32))

    total = last(0) + last(1)
    gains[me] = total.sum(0, keepdims=True)

    def tell(n, slot):
        to = lax.rem(me + n, DEVICES)
        return pltpu.make_async_remote_copy(src_ref=gains.at[slot], dst_ref=gains.at[slot], send_sem=gsend.at[n], recv_sem=grecv.at[n],
                                            device_id={"tp": to}, device_id_type=MESH)
    for n in range(1, DEVICES):
        tell(n, me).start()
    done = pltpu.make_async_copy(dys.at[5], dx_ref, lsem.at[7])
    done.start()
    for to in range(2):
        for quarter in range(2):
            to_x(to, quarter).wait_send()
            to_y(to, quarter).wait_send()
        round_x(to).wait_send()
        round_y(to).wait_send()
    for n in range(1, DEVICES):
        tell(n, lax.rem(me - n + 8, 8)).wait_recv()
    dgain_ref[...] = gains[...].sum(0)
    for n in range(1, DEVICES):
        tell(n, me).wait_send()
    for c in (*results, done, by_wo):
        c.wait()


def layer_stage(x, dy, gain, wq, wk, wv, wo):
    n = DEVICES
    tables = [jnp.asarray(t) for t in rotary_tables(n)]
    rows, d = n * BLK, x.shape[1]
    hbm, vmem = pl.BlockSpec(memory_space=pl.ANY), pl.BlockSpec(memory_space=pltpu.VMEM)
    low, f32 = jnp.bfloat16, jnp.float32
    sds, sem, room = jax.ShapeDtypeStruct, pltpu.SemaphoreType.DMA, pltpu.VMEM
    return pl.pallas_call(
        layer_kernel,
        out_shape=[sds((n, BLK, d), low), sds((BLK, d), low), sds((1, d), f32), sds((d, WIDE), low), sds((d, HEAD), low), sds((d, HEAD), low),
                   sds((WIDE, d), low)],
        in_specs=[hbm, hbm, vmem, hbm, hbm, hbm, hbm, vmem, vmem, vmem, vmem],
        out_specs=[hbm, hbm, vmem, hbm, hbm, hbm, hbm],
        scratch_shapes=[room((n, BLK, d), low), room((n, BLK, d), low), room((2, BLK, d), low),
                        room((2, rows, HEAD), low), room((rows, HEAD), low), room((rows, HEAD), low), room((2, rows, HEAD), low), room((n, 2 * BLK), f32), room((n, 2 * BLK), f32), room((WIDE, d), f32), room((4, BLK), f32),
                        room((d, 4 * HEAD), f32), room((rows, HEAD), f32), room((rows, HEAD), f32), room((n, 1, d), f32),
                        sem((8,)), sem((2,)), sem((2, 7, PIECES)), sem((2, 7, PIECES)), sem((4, 8)), sem((4, 8)), sem((n,)), sem((n,)),
                        pltpu.SemaphoreType.REGULAR],
        compiler_params=pltpu.CompilerParams(collective_id=0, has_side_effects=True, vmem_limit_bytes=67043328),
        name="layer_stage",
    )(x, dy, gain[None], wq, wk, wv, wo, *tables)


def hand_on(*refs):
    sems = refs[-1]
    n = len(refs) // 3
    given, results, buffers = refs[:n], refs[n : n + n], refs[n + n : -1]
    ins = [pltpu.make_async_copy(given[i], buffers[i], sems.at[0, i]) for i in range(n)]
    outs = [pltpu.make_async_copy(buffers[i], results[i], sems.at[1, i]) for i in range(n)]
    for c in ins:
        c.start()
    for c, o in zip(ins, outs):
        c.wait()
        o.start()
    for o in outs:
        o.wait()


def solution(mesh):
    def step(x, dy, gain, wq, wk, wv, wo):
        got = layer_stage(x, dy, gain, wq, wk, wv, wo)[1:]
        hbm = pl.BlockSpec(memory_space=pl.ANY)
        return tuple(pl.pallas_call(
            hand_on,
            out_shape=[jax.ShapeDtypeStruct(t.shape, t.dtype) for t in got],
            in_specs=[hbm for t in got],
            out_specs=[hbm for t in got],
            scratch_shapes=[*[pltpu.VMEM(t.shape, t.dtype) for t in got], pltpu.SemaphoreType.DMA((2, len(got)))],
            name="hand_on",
        )(*got))

    tokens, columns = P(("dp", "tp"), None), P(None, "tp")
    return jax.shard_map(
        step,
        mesh=mesh,
        in_specs=(tokens, tokens, P(None), columns, columns, columns, P("tp", None)),
        out_specs=(tokens, P("dp", None), P("dp", "tp"), P("dp", "tp"), P("dp", "tp"), P(("dp", "tp"), None)),
        check_vma=False,
    )
```

```python
import jax
import jax.numpy as jnp
import numpy as np
from jax import lax
from jax.experimental import pallas as pl
from jax.experimental.pallas import tpu as pltpu
from jax.sharding import PartitionSpec as P

NEG = -1e30
HIDDEN = 2 * NEG
LOG2E = 1.4426950408889634
HEAD = 128
THETA = 10000
MESH = pl.DeviceIdType.MESH
UNROLL = 2
DEVICES = 8
WIDE = 2 * HEAD
BLK = 512
MIX = HEAD + 8
PIECES = 8
EPS = 1e-6
SCALE = HEAD**-0.5
E = SCALE * LOG2E


def _dot(a, b, ca, cb):
    return lax.dot_general(a, b, (((ca,), (cb,)), ((), ())), preferred_element_type=jnp.float32)


def dot(a, b):
    return _dot(a, b, 1, 0)


def dot_rows(a, b):
    return _dot(a, b, 1, 1)


def dot_columns(a, b):
    return _dot(a, b, 0, 0)


def pair_of(n):
    return lax.div(n, 2)


def parity(n):
    return lax.rem(n, 2)


def repeat(times, body, unroll=1):
    lax.fori_loop(0, times, body, None, unroll=unroll)


def flip(me, bit):
    return me + bit - 2 * bit * parity(lax.div(me, bit))


def rotary_tables(n):
    half = HEAD // 2
    rate = np.float64(np.float32(THETA) ** (-np.arange(half, dtype=np.float32) / np.float32(half)))
    rate = np.concatenate([rate, rate])[None]
    inner, outer = np.arange(BLK)[:, None] * rate, (BLK * np.arange(n))[:, None] * rate
    return [f(t).astype(np.float32) for t in (inner, outer) for f in (np.cos, np.sin)]


TURNS = (0, 7, 2, 5, 1, 6, 3, 4)
HALF = BLK // 2
QUARTER = BLK // 4
AHEAD = 1


def turn_at(n):
    got = jnp.int32(TURNS[0])
    for i in range(1, len(TURNS)):
        got = jnp.where(n == i, TURNS[i], got)
    return got


def layer_kernel(x_ref, dy_ref, gain_ref, wq_ref, wk_ref, wv_ref, wo_ref, ci_ref, si_ref, co_ref, so_ref,
                 a_ref, dx_ref, dgain_ref, dwq_ref, dwk_ref, dwv_ref, dwo_ref,
                 xs, dys, stage, q_s, k_s, v_s, do_s, lse_s, delta_s, wide_s, top_s, dq_s, dk_s, dv_s, gains,
                 lsem, asem, ssem, rsem, ssem2, rsem2, gsend, grecv, ready):
    low, f32 = jnp.bfloat16, jnp.float32
    d = x_ref.shape[1]
    me = lax.axis_index("tp")
    sib, yn, xn = flip(me, 1), flip(me, 2), flip(me, 4)
    dg = flip(yn, 4)
    rows = BLK // PIECES
    barrier = pltpu.get_barrier_semaphore()
    for n in range(1, DEVICES):
        pl.semaphore_signal(barrier, inc=1, device_id={"tp": lax.rem(me + n, DEVICES)}, device_id_type=MESH)
    loads = [pltpu.make_async_copy(x_ref, xs.at[me], lsem.at[0]), pltpu.make_async_copy(dy_ref, dys.at[me], lsem.at[1]),
             pltpu.make_async_copy(wq_ref.at[:, pl.ds(0, HEAD)], do_s.at[0, pl.ds(0, d)], lsem.at[2]),
             pltpu.make_async_copy(wq_ref.at[:, pl.ds(HEAD, HEAD)], do_s.at[0, pl.ds(d, d)], lsem.at[3]),
             pltpu.make_async_copy(wk_ref, do_s.at[1, pl.ds(0, d)], lsem.at[4]),
             pltpu.make_async_copy(wv_ref, do_s.at[1, pl.ds(d, d)], lsem.at[5])]
    for c in loads:
        c.start()
    pl.semaphore_wait(barrier, 7)
    loads[0].wait()

    def copy(buf, n, kind, owner, p, to):
        part = buf.at[owner, pl.ds(p * rows, rows)]
        return pltpu.make_async_remote_copy(src_ref=part, dst_ref=part, send_sem=ssem.at[n, kind, p], recv_sem=rsem.at[n, kind, p],
                                            device_id={"tp": to}, device_id_type=MESH)

    def send_own(buf, n, p):
        copy(buf, n, 1, me, p, xn).start()
        copy(buf, n, 2, me, p, yn).start()

    def send_sib(buf, n):
        def go(p, _):
            copy(buf, n, 0, me, p, sib).start()
        repeat(PIECES, go)

    def pass_on(buf, n, p):
        copy(buf, n, 1, xn, p, xn).wait_recv()
        copy(buf, n, 3, xn, p, sib).start()

        @pl.when(parity(p) == 0)
        def _():
            copy(buf, n, 5, xn, p, yn).start()

        copy(buf, n, 2, yn, p, yn).wait_recv()
        copy(buf, n, 4, yn, p, sib).start()

        @pl.when(parity(p) == 1)
        def _():
            copy(buf, n, 5, yn, p, xn).start()

    def pass_diagonal(buf, n, p):
        copy(buf, n, 5, dg, p, xn).wait_recv()
        copy(buf, n, 6, dg, p, sib).start()

    def arrived(buf, n, kind, owner):
        def go(p, _):
            copy(buf, n, kind, owner, p, sib).wait_recv()
        repeat(PIECES, go)

    def owner_at(t):
        base = jnp.where(t < 2, me, jnp.where(t < 6, jnp.where(parity(t) == 0, xn, yn), dg))
        other = jnp.where(t < 2, t == 1, jnp.where(t < 6, t >= 4, t == 7))
        return jnp.where(other, flip(base, 1), base)

    def await_block(buf, n, t):
        @pl.when(t == 1)
        def _():
            arrived(buf, n, 0, sib)

        @pl.when((t >= 3 - n) & (t < 7 - n))
        def _():
            for u in range(2):
                pass_diagonal(buf, n, 2 * (t - 3 + n) + u)

        @pl.when(t == 4)
        def _():
            arrived(buf, n, 3, flip(xn, 1))

        @pl.when(t == 5)
        def _():
            arrived(buf, n, 4, flip(yn, 1))

        @pl.when(t == 7)
        def _():
            arrived(buf, n, 6, flip(dg, 1))

    def first(p, _):
        send_own(xs, 0, p)
    repeat(PIECES, first)
    send_sib(xs, 0)
    for c in loads[1:]:
        c.wait()

    def put(t):
        slot = parity(t)
        return pltpu.make_async_copy(stage.at[slot], a_ref.at[owner_at(t)], asem.at[slot])

    def project(t, _):
        @pl.when(t == 2)
        def _():
            def go(p, _):
                pass_on(xs, 0, p)
            repeat(PIECES, go)

        await_block(xs, 0, t)

        @pl.when((t >= 2) & (t < 6))
        def _():
            for u in range(2):
                send_own(dys, 1, 2 * (t - 2) + u)

        @pl.when(t >= 2)
        def _():
            put(t - 2).wait()

        owner, slot = owner_at(t), parity(t)
        gain = gain_ref[...].astype(f32)

        def norm(i, _):
            here = pl.ds(i * 64, 64)
            wide = xs[owner, here, :].astype(jnp.float32)
            s = lax.rsqrt(jnp.mean(wide * wide, -1, keepdims=True) + EPS)
            stage[slot, here, :] = (wide * s * gain).astype(jnp.bfloat16)
        repeat(BLK // 64, norm)

        def multiply(i, _):
            here = pl.ds(pl.multiple_of(i * HALF, HALF), HALF)
            there = pl.ds(pl.multiple_of(owner * BLK + i * HALF, HALF), HALF)
            w = jnp.concatenate([do_s[h, n * d : (n + 1) * d, :] for h in range(2) for n in range(2)], axis=1)
            got = dot(stage[slot, here, :], w)
            co, so = co_ref[pl.ds(owner, 1), :], so_ref[pl.ds(owner, 1), :]
            ci, si = ci_ref[here, :], si_ref[here, :]
            sign = jnp.where(lax.broadcasted_iota(jnp.int32, (1, HEAD), 1) < HEAD // 2, -1.0, 1.0)
            cos, sin = ci * co - si * so, (si * co + ci * so) * sign

            def turned(z):
                z = z.astype(jnp.bfloat16).astype(jnp.float32)
                return (z * cos + pltpu.roll(z, HEAD // 2, 1) * sin).astype(jnp.bfloat16)
            q_s[0, there, :] = turned(got[:, :HEAD])
            q_s[1, there, :] = turned(got[:, HEAD : WIDE])
            k_s[there, :] = turned(got[:, WIDE : 3 * HEAD])
            v_s[there, :] = got[:, 3 * HEAD :].astype(jnp.bfloat16)
        repeat(BLK // HALF, multiply)
        put(t).start()
    repeat(DEVICES, project)
    send_sib(dys, 1)

    def drain(n, buf):
        def go(p, _):
            for kind in range(7):
                copy(buf, n, kind, me, p, sib).wait_send()
        repeat(PIECES, go)
    drain(0, xs)
    for t in (sib, xn, yn, flip(xn, 1), flip(yn, 1)):
        pl.semaphore_signal(ready, inc=1, device_id={"tp": t}, device_id_type=MESH)
    for t in (6, 7):
        put(t).wait()
    get_wo = pltpu.make_async_copy(wo_ref, stage.at[0, pl.ds(0, WIDE)], lsem.at[0])
    get_wo.start()

    ones = jnp.ones((8, BLK), jnp.bfloat16)

    def attend_rows(r, _):
        top_s[...] = jnp.full(top_s.shape, NEG, jnp.float32)
        dq_s[: 4 * MIX, :] = jnp.zeros((4 * MIX, BLK), f32)

        def block(j, strips, masked):
            here = pl.ds(pl.multiple_of(j * BLK, BLK), BLK)
            keys = k_s[here, :]
            values = jnp.concatenate([v_s[here, :].T, ones], axis=0)
            scores = [dot_rows(keys, q_s[h, pl.ds(pl.multiple_of(r * 2 * BLK + half * BLK, BLK), BLK), :]) for h, half in strips]
            weights, keeps = [], []
            for (h, half), s in zip(strips, scores):
                n = 2 * h + half
                if half in masked:
                    seen = lax.broadcasted_iota(jnp.int32, (BLK, BLK), 0) <= lax.broadcasted_iota(jnp.int32, (BLK, BLK), 1)
                    s = jnp.where(seen, s, HIDDEN)
                old = top_s[n : n + 1, :]
                top = jnp.maximum(old, s.max(axis=0, keepdims=True))
                top_s[n : n + 1, :] = top
                weights.append(jnp.exp2((s - top) * E).astype(jnp.bfloat16))
                keeps.append(jnp.exp2((old - top) * E))
            for (h, half), p, keep in zip(strips, weights, keeps):
                n = 2 * h + half
                here = pl.ds(n * MIX, MIX)
                dq_s[here, :] = dq_s[here, :] * keep + dot(values, p)

        every = [(0, 0), (0, 1), (1, 0), (1, 1)]
        lax.fori_loop(0, 2 * r, lambda j, _: block(j, every, ()), None)
        block(2 * r, every, (0,))
        block(2 * r + 1, [(0, 1), (1, 1)], (1,))
        for h, half in every:
            n = 2 * h + half
            total = dq_s[n * MIX + HEAD : n * MIX + HEAD + 1, :]
            xs[7, :, pl.ds(pl.multiple_of((2 * r + half) * WIDE + h * HEAD, HEAD), HEAD)] = (dq_s[n * MIX : n * MIX + HEAD, :] * (1 / total)).T.astype(jnp.bfloat16)
            lse_s[pl.ds(2 * r + half, 1), h * BLK : (h + 1) * BLK] = top_s[n : n + 1, :] * E + jnp.log2(total)
        pass_on(dys, 1, r)
    repeat(4, attend_rows)

    get_wo.wait()
    def transpose(i, _):
        here = pl.ds(pl.multiple_of(i * HALF, HALF), HALF)
        for n in range(4):
            stage[1, n * HEAD : (n + 1) * HEAD, here] = do_s[n // 2, pl.ds(pl.multiple_of(n % 2 * d + i * HALF, HALF), HALF), :].T
    repeat(d // HALF, transpose)

    dq_s[...] = jnp.zeros(dq_s.shape, f32)
    dk_s[...] = jnp.zeros(dk_s.shape, f32)
    dv_s[...] = jnp.zeros(dv_s.shape, f32)
    wide_s[...] = jnp.zeros(wide_s.shape, f32)

    def at(block):
        return pl.ds(pl.multiple_of(block * BLK, BLK), BLK)

    def rows_of(block, part):
        return pl.ds(pl.multiple_of(block * BLK + part[0], HALF), part[1])

    def pieces(*todo):
        work = [(h, n) for n in range(len(todo)) for h in range(2)]
        keys = [k_s[rows_of(kb, kp), :] for _, kb, _, kp, _ in todo]
        values = [v_s[rows_of(kb, kp), :] for _, kb, _, kp, _ in todo]
        qs = [q_s[h, rows_of(todo[n][0], todo[n][2]), :] for h, n in work]
        dos = [do_s[h, rows_of(todo[n][0], todo[n][2]), :] for h, n in work]
        def products(i):
            h, n = work[i]
            return dot_rows(keys[n], qs[i]), dot_rows(values[n], dos[i])

        ready_at = [products(i) for i in range(min(AHEAD, len(work)))]
        for i, (h, n) in enumerate(work):
            if i + AHEAD < len(work):
                ready_at.append(products(i + AHEAD))
            s, dp = ready_at[i]
            ready_at[i] = None
            qb, kb, qp, kp, masked = todo[n]
            columns = pl.ds(h * BLK + qp[0], qp[1])
            p = jnp.exp2(s * E - lse_s[pl.ds(qb, 1), columns])
            if masked:
                seen = lax.broadcasted_iota(jnp.int32, s.shape, 0) + kp[0] <= lax.broadcasted_iota(jnp.int32, s.shape, 1) + qp[0]
                p = jnp.where(seen, p, 0.0)
            ds = (p * (dp - delta_s[pl.ds(qb, 1), columns])).astype(low)
            p = p.astype(low)
            dq_s[pl.ds(pl.multiple_of(qb * WIDE + h * HEAD, HEAD), HEAD), qp[0] : qp[0] + qp[1]] += dot(keys[n].T, ds)
            here = rows_of(kb, kp)
            dv_s[here, :] += dot(p, dos[i])
            dk_s[here, :] += dot(ds, qs[i])

    whole, upper, lower = (0, BLK), (0, HALF), (HALF, HALF)

    def two_blocks(a, b):
        pieces((*a, whole, whole, False), (*b, whole, whole, False))

    def one_block(q, k):
        pieces((q, k, whole, upper, False), (q, k, whole, lower, False))

    def diagonal_block(i):
        pieces((i, i, whole, upper, True), (i, i, lower, lower, True))

    def early(block):
        return (pair_of(block) == pair_of(me)) | (me < 4) & (block < 4) | (me < 2) & (block == 4) | (pair_of(me) == 2) & (block < 2)

    def back_out(t, _):
        @pl.when(t == 0)
        def _():
            pass_on(dys, 1, 4)

        @pl.when(t == 1)
        def _():
            pass_on(dys, 1, 5)

        @pl.when(t == 2)
        def _():
            pass_on(dys, 1, 6)
            pass_on(dys, 1, 7)
        await_block(dys, 1, t)
        owner = owner_at(t)
        there = at(owner)
        got = dot_rows(dys[owner], stage[0, : WIDE, :]).astype(low)
        o = xs[7, :, pl.ds(pl.multiple_of(owner * WIDE, WIDE), WIDE)]
        prod = got.astype(f32) * o.astype(f32)
        for h in range(2):
            do_s[h, there, :] = got[:, h * HEAD : (h + 1) * HEAD]
            delta_s[pl.ds(owner, 1), h * BLK : (h + 1) * BLK] = prod[:, h * HEAD : (h + 1) * HEAD].T.sum(axis=0, keepdims=True)
        wide_s[...] += dot_columns(o, dys[owner])

        @pl.when(early(owner))
        def _():
            def two(m, _):
                two_blocks((owner, 2 * m), (owner, 2 * m + 1))
            repeat(pair_of(owner), two)

            @pl.when(parity(owner) == 1)
            def _():
                one_block(owner, owner - 1)
            diagonal_block(owner)
    repeat(DEVICES, back_out)
    drain(1, dys)
    stage[0, : WIDE, :] = wide_s[...].astype(low)
    pl.semaphore_wait(ready, 5)
    by_wo = pltpu.make_async_copy(stage.at[0, pl.ds(0, WIDE)], dwo_ref, lsem.at[4])
    mine = [pltpu.make_async_copy(x_ref, dys.at[4], lsem.at[5]), pltpu.make_async_copy(dy_ref, dys.at[5], lsem.at[6])]
    for c in (by_wo, *mine):
        c.start()

    def part(i, n):
        return pl.ds(pl.multiple_of(lax.rem(i, 4) * BLK + n * HEAD, HEAD), HEAD)

    def all_of(i):
        return pl.ds(pl.multiple_of(lax.rem(i, 4) * BLK, BLK), BLK)

    def finish(i):
        co, so = co_ref[pl.ds(i, 1), :], so_ref[pl.ds(i, 1), :]
        ci, si = ci_ref[...], si_ref[...]
        sign = jnp.where(lax.broadcasted_iota(jnp.int32, (1, HEAD), 1) < HEAD // 2, -1.0, 1.0)
        cos, sin = ci * co - si * so, (si * co + ci * so) * sign

        def turned_back(z):
            z = z * SCALE
            return (z * cos + pltpu.roll(z * sin, HEAD // 2, 1)).astype(low)
        for h in range(2):
            rows = pl.ds(pl.multiple_of(i * WIDE + h * HEAD, HEAD), HEAD)
            dys[lax.div(i, 4), :, part(i, h)] = turned_back(dq_s[rows, :].T)
        dys[lax.div(i, 4), :, part(i, 2)] = turned_back(dk_s[at(i), :])
        dys[lax.div(i, 4), :, part(i, 3)] = dv_s[at(i), :].astype(low)

    core = parity(me)

    def where(i):
        there, here = pair_of(i), pair_of(me)
        far_x = parity(pair_of(there) + pair_of(here))
        far_y = parity(there + here)
        return 2 * far_x + far_y, parity(i)

    def half_rows(half):
        return pl.ds(pl.multiple_of(half * HALF, HALF), HALF)

    def quarter_rows(half, quarter):
        return pl.ds(pl.multiple_of(half * HALF + quarter * QUARTER, QUARTER), QUARTER)

    def term(i, rows, put):
        def go(c, _):
            columns = pl.ds(pl.multiple_of(c * BLK, BLK), BLK)
            put(columns, dot(dys[lax.div(i, 4), rows, all_of(i)], stage[1, :, columns]))
        repeat(d // BLK, go, UNROLL)

    def sum_copy(kind, src, dst, left_n, n, to):
        return pltpu.make_async_remote_copy(src_ref=src, dst_ref=dst, send_sem=ssem2.at[kind, left_n], recv_sem=rsem2.at[kind, n],
                                            device_id={"tp": to}, device_id_type=MESH)

    def to_sib(slot, half, place, landing):
        return sum_copy(0, dys.at[6 + slot, half_rows(half)], xs.at[place, half_rows(landing)], 2 * place + landing, 2 * place + landing, sib)

    def kept_by(neighbour, to):
        return pair_of(neighbour) * 2 + to

    def to_x(to, quarter):
        return sum_copy(1, xs.at[2, quarter_rows(to, quarter)], xs.at[4, quarter_rows(core, quarter)], 2 * to + quarter, 2 * core + quarter, kept_by(xn, to))

    def to_y(to, quarter):
        return sum_copy(2, xs.at[1, quarter_rows(to, quarter)], xs.at[5, quarter_rows(core, quarter)], 2 * to + quarter, 2 * core + quarter, kept_by(yn, to))

    def from_x(half, quarter):
        return sum_copy(1, xs.at[2, quarter_rows(half, quarter)], xs.at[4, quarter_rows(half, quarter)], 0, 2 * half + quarter, xn)

    def from_y(half, quarter):
        return sum_copy(2, xs.at[1, quarter_rows(half, quarter)], xs.at[5, quarter_rows(half, quarter)], 0, 2 * half + quarter, yn)

    def round_x(to):
        return sum_copy(3, xs.at[3, quarter_rows(to, 0)], xs.at[6, quarter_rows(to, 0)], 2 * to, 2 * to, xn)

    def round_y(to):
        return sum_copy(3, xs.at[3, quarter_rows(to, 1)], xs.at[6, quarter_rows(to, 1)], 2 * to + 1, 2 * to + 1, yn)

    def offer(t):
        i = turn_at(t)
        place, to = where(i)
        slot = parity(t)

        def give(half, landing):
            def put(columns, z):
                dys[6 + slot, half_rows(half), columns] = z.astype(low)
            term(i, half_rows(half), put)
            to_sib(slot, half, place, landing).start()

        @pl.when(place > 0)
        def _():
            give(1 - core, to)

        @pl.when((place == 0) & (to != core))
        def _():
            def both(half, _):
                give(half, half)
            repeat(2, both)

    def left(t):
        place, to = where(turn_at(t))

        @pl.when(place > 0)
        def _():
            to_sib(0, 0, place, to).wait_send()

        @pl.when((place == 0) & (to != core))
        def _():
            for half in range(2):
                to_sib(0, 0, 0, half).wait_send()

    def add(i, place, to, quarter, relayed):
        def put(columns, z):
            here = quarter_rows(to, quarter)
            z = z + xs[place, here, columns].astype(f32)
            if relayed:
                z = z + xs[6, here, columns].astype(f32)
            xs[place, here, columns] = z.astype(low)
        term(i, quarter_rows(core, quarter), put)

    LATE = DEVICES // 2

    def gather_sum(t):
        i = turn_at(t)
        place, to = where(i)

        @pl.when(place == 3)
        def _():
            to_sib(0, 0, place, to).wait_recv()

            def put(columns, z):
                xs[3, half_rows(to), columns] = (z + xs[3, half_rows(to), columns].astype(f32)).astype(low)
            term(i, half_rows(core), put)
            round_x(to).start()
            round_y(to).start()

        @pl.when(t < LATE)
        def _():
            direct_sum(t)

    def direct_sum(t):
        i = turn_at(t)
        place, to = where(i)

        @pl.when((place == 1) | (place == 2))
        def _():
            to_sib(0, 0, place, to).wait_recv()

        @pl.when(place == 1)
        def _():
            add(i, 1, to, 1, False)
            to_y(to, 1).start()

        @pl.when(place == 2)
        def _():
            add(i, 2, to, 0, False)
            to_x(to, 0).start()

    def pass_sum(t):
        i = turn_at(t)
        place, to = where(i)

        @pl.when(place == 1)
        def _():
            round_x(to).wait_recv()
            add(i, 1, to, 0, True)
            to_y(to, 0).start()

        @pl.when(place == 2)
        def _():
            round_y(to).wait_recv()
            add(i, 2, to, 1, True)
            to_x(to, 1).start()

    def turn(t, _):
        i = turn_at(t)

        @pl.when(jnp.logical_not(early(i)))
        def _():
            diagonal_block(i)

        def pair_with(c):
            return jnp.maximum(i, c), jnp.minimum(i, c)

        def others(m, held):
            c = turn_at(m)
            wanted = jnp.logical_not(early(jnp.maximum(i, c)))

            @pl.when(wanted & (held >= 0))
            def _():
                two_blocks(pair_with(held), pair_with(c))

            @pl.when((t >= 1) & (m == t + 3))
            def _():
                gather_sum(t - 1)
            return jnp.where(wanted, jnp.where(held >= 0, -1, c), held)
        held = lax.fori_loop(t + 1, DEVICES, others, jnp.int32(-1))

        @pl.when(held >= 0)
        def _():
            one_block(*pair_with(held))

        @pl.when(t >= 5)
        def _():
            gather_sum(t - 1)
        finish(i)

        @pl.when(t >= 2)
        def _():
            left(t - 2)
        offer(t)

        @pl.when((t >= 2) & (t < 7) & (parity(t) == 0))
        def _():
            pass_sum(pair_of(t) - 1)
    repeat(DEVICES, turn)

    def load(n):
        return pltpu.make_async_copy(a_ref.at[n], dys.at[2 + parity(n)], asem.at[parity(n)])

    load(0).start()
    gather_sum(jnp.int32(7))
    pass_sum(3)

    def rest(n, _):
        direct_sum(LATE + n)
    repeat(LATE, rest)
    dq_s[...] = jnp.zeros(dq_s.shape, f32)

    def weights(n, _):
        @pl.when(n < 7)
        def _():
            load(n + 1).start()

        @pl.when((n >= 1) & (n < 5))
        def _():
            pass_sum(n + 3)
        load(n).wait()

        def go(c, _):
            rows = pl.ds(pl.multiple_of(c * BLK, BLK), BLK)
            dq_s[rows, :] += dot_columns(dys[2 + parity(n), :, rows], dys[lax.div(n, 4), :, all_of(n)])
        repeat(d // BLK, go)
    repeat(DEVICES, weights)
    for n, half in enumerate((q_s.at[0], q_s.at[1], k_s, v_s)):
        half[:d, :] = dq_s[:, n * HEAD : (n + 1) * HEAD].astype(low)
    results = [pltpu.make_async_copy(q_s.at[0, pl.ds(0, d)], dwq_ref.at[:, pl.ds(0, HEAD)], lsem.at[0]),
               pltpu.make_async_copy(q_s.at[1, pl.ds(0, d)], dwq_ref.at[:, pl.ds(HEAD, HEAD)], lsem.at[1]),
               pltpu.make_async_copy(k_s.at[pl.ds(0, d)], dwk_ref, lsem.at[2]), pltpu.make_async_copy(v_s.at[pl.ds(0, d)], dwv_ref, lsem.at[3])]
    left(6)
    left(7)
    for c in results:
        c.start()
    for c in mine:
        c.wait()
    gain = gain_ref[...].astype(f32)

    def last(half):
        to_sib(0, 0, 0, half).wait_recv()
        for quarter in range(2):
            from_x(half, quarter).wait_recv()
            from_y(half, quarter).wait_recv()

        def add_up(columns, z):
            wide_s[:, columns] = z + sum(xs[n, half_rows(half), columns].astype(f32) for n in (0, 4, 5))
        term(me, half_rows(half), add_up)

        def go(r, total):
            here, there = pl.ds(pl.multiple_of(r * 32, 32), 32), pl.ds(pl.multiple_of(half * HALF + r * 32, 32), 32)
            da = wide_s[here, :]
            wide = dys[4, there, :].astype(f32)
            s = lax.rsqrt(jnp.mean(wide * wide, -1, keepdims=True) + EPS)
            hat = wide * s
            by_hat = da * hat
            z = da * gain
            dx = s * (z - hat * jnp.mean(z * hat, -1, keepdims=True))
            dys[5, there, :] = (dx + dys[5, there, :].astype(f32)).astype(low)
            return total + by_hat.reshape(4, 8, d).sum(0)
        return lax.fori_loop(0, HALF // 32, go, jnp.zeros((8, d), f32))

    total = last(0) + last(1)
    gains[me] = total.sum(0, keepdims=True)

    def tell(n, slot):
        to = lax.rem(me + n, DEVICES)
        return pltpu.make_async_remote_copy(src_ref=gains.at[slot], dst_ref=gains.at[slot], send_sem=gsend.at[n], recv_sem=grecv.at[n],
                                            device_id={"tp": to}, device_id_type=MESH)
    for n in range(1, DEVICES):
        tell(n, me).start()
    done = pltpu.make_async_copy(dys.at[5], dx_ref, lsem.at[7])
    done.start()
    for to in range(2):
        for quarter in range(2):
            to_x(to, quarter).wait_send()
            to_y(to, quarter).wait_send()
        round_x(to).wait_send()
        round_y(to).wait_send()
    for n in range(1, DEVICES):
        tell(n, lax.rem(me - n + 8, 8)).wait_recv()
    dgain_ref[...] = gains[...].sum(0)
    for n in range(1, DEVICES):
        tell(n, me).wait_send()
    for c in (*results, done, by_wo):
        c.wait()


def layer_stage(x, dy, gain, wq, wk, wv, wo):
    n = DEVICES
    tables = [jnp.asarray(t) for t in rotary_tables(n)]
    rows, d = n * BLK, x.shape[1]
    hbm, vmem = pl.BlockSpec(memory_space=pl.ANY), pl.BlockSpec(memory_space=pltpu.VMEM)
    low, f32 = jnp.bfloat16, jnp.float32
    sds, sem, room = jax.ShapeDtypeStruct, pltpu.SemaphoreType.DMA, pltpu.VMEM
    return pl.pallas_call(
        layer_kernel,
        out_shape=[sds((n, BLK, d), low), sds((BLK, d), low), sds((1, d), f32), sds((d, WIDE), low), sds((d, HEAD), low), sds((d, HEAD), low),
                   sds((WIDE, d), low)],
        in_specs=[hbm, hbm, vmem, hbm, hbm, hbm, hbm, vmem, vmem, vmem, vmem],
        out_specs=[hbm, hbm, vmem, hbm, hbm, hbm, hbm],
        scratch_shapes=[room((n, BLK, d), low), room((n, BLK, d), low), room((2, BLK, d), low),
                        room((2, rows, HEAD), low), room((rows, HEAD), low), room((rows, HEAD), low), room((2, rows, HEAD), low), room((n, 2 * BLK), f32), room((n, 2 * BLK), f32), room((WIDE, d), f32), room((4, BLK), f32),
                        room((d, 4 * HEAD), f32), room((rows, HEAD), f32), room((rows, HEAD), f32), room((n, 1, d), f32),
                        sem((8,)), sem((2,)), sem((2, 7, PIECES)), sem((2, 7, PIECES)), sem((4, 8)), sem((4, 8)), sem((n,)), sem((n,)),
                        pltpu.SemaphoreType.REGULAR],
        compiler_params=pltpu.CompilerParams(collective_id=0, has_side_effects=True, vmem_limit_bytes=67043328),
        name="layer_stage",
    )(x, dy, gain[None], wq, wk, wv, wo, *tables)


def hand_on(*refs):
    sems = refs[-1]
    n = len(refs) // 3
    given, results, buffers = refs[:n], refs[n : n + n], refs[n + n : -1]
    ins = [pltpu.make_async_copy(given[i], buffers[i], sems.at[0, i]) for i in range(n)]
    outs = [pltpu.make_async_copy(buffers[i], results[i], sems.at[1, i]) for i in range(n)]
    for c in ins:
        c.start()
    for c, o in zip(ins, outs):
        c.wait()
        o.start()
    for o in outs:
        o.wait()


def solution(mesh):
    def step(x, dy, gain, wq, wk, wv, wo):
        got = layer_stage(x, dy, gain, wq, wk, wv, wo)[1:]
        hbm = pl.BlockSpec(memory_space=pl.ANY)
        return tuple(pl.pallas_call(
            hand_on,
            out_shape=[jax.ShapeDtypeStruct(t.shape, t.dtype) for t in got],
            in_specs=[hbm for t in got],
            out_specs=[hbm for t in got],
            scratch_shapes=[*[pltpu.VMEM(t.shape, t.dtype) for t in got], pltpu.SemaphoreType.DMA((2, len(got)))],
            name="hand_on",
        )(*got))

    tokens, columns = P(("dp", "tp"), None), P(None, "tp")
    return jax.shard_map(
        step,
        mesh=mesh,
        in_specs=(tokens, tokens, P(None), columns, columns, columns, P("tp", None)),
        out_specs=(tokens, P("dp", None), P("dp", "tp"), P("dp", "tp"), P("dp", "tp"), P(("dp", "tp"), None)),
        check_vma=False,
    )
```
